32 devices in a mesh: ctx: 8 (over y, x, core), head: 4 (over z).
Axes of the slice: x: 2, y: 2, z: 4, core: 2. Of those that a mesh axis runs over, the one named last changes fastest.
Arguments:
- q_latent: bfloat16 [2048, 1536], P('ctx', 'head'), may hold values from -70 to 70
- kv_latent: bfloat16 [2048, 576], P('ctx', 'head'), may hold values from -6 to 6
- w_query: bfloat16 [1536, 12288], P(None, 'head'), may hold values from -0.15625 to 0.15625
- w_key: bfloat16 [512, 8192], P(None, 'head'), may hold values from -0.25 to 0.25
- w_value: bfloat16 [512, 8192], P(None, 'head'), may hold values from -0.25 to 0.25
- d_out: bfloat16 [2048, 8192], P('ctx', 'head'), may hold values from -6 to 6
Outputs:
- attn_out: bfloat16 [2048, 8192], P('ctx', 'head')
- grad_qlat: float32 [2048, 1536], P('ctx', 'head')
- grad_kvlat: float32 [2048, 576], P('ctx', 'head')
The draws below stay inside these ranges and needn't reach their ends.
All inputs are finite; a program needn't handle non-finite values.
Results may differ from the reference program's by a relative error of at most 0.023.
The reference program's roundings to bfloat16 on the way (of `queries`, `probs_b`, `dscore` and `grad_query`) count: a program that leaves them out, or rounds other values in their place, can miss the bound.
Values may be sent and summed in bfloat16 or wider, within the bound.
A program may use at most 128 MiB of HBM per device.

```python
import jax
import jax.numpy as jnp
from jax import lax

QL = 1536
KVL = 512
ROPE = 64
NOPE = 128
VDIM = 128
HEAD_DEV = 16
TOK_DEV = 256
HEADS = 64
TOKENS = 2048
N_CTX = 8
N_HEAD = 4


def draw_q_latent(key, part):
    base_key = jax.random.fold_in(jax.random.fold_in(key, 11), 0)
    values = jax.random.normal(base_key, (TOKENS, QL), jnp.float32)
    return jnp.clip(values, -6.0, 6.0).astype(jnp.bfloat16)


def steps_of(key, dims, shards, low, high):
    def one(axis_at, parts):
        heights = jax.random.uniform(jax.random.fold_in(jax.random.fold_in(key, 6), axis_at), (parts,), jnp.float32, low / len(shards), high / len(shards))
        return jnp.repeat(jnp.exp(heights), dims[axis_at] // parts).reshape((-1,) + (1,) * (len(dims) - axis_at - 1))

    factor_of = one(*shards[0])
    for cut in shards[1:]:
        factor_of = factor_of * one(*cut)
    return factor_of


def noise(stream_key, dims, deviation, reach, cuts=(), held_as=jnp.bfloat16):
    loudness = steps_of(stream_key, dims, cuts, -0.22, 0.18) if cuts else 1.0
    result = jax.random.normal(stream_key, dims, jnp.float32) * deviation * loudness
    return jnp.minimum(jnp.maximum(result, -reach), reach).astype(held_as)


def setup_inputs(seed: int = 0) -> dict:
    streams_of = jax.random.split(jax.random.key(seed), 7)
    return {
        "q_latent": draw_q_latent(jax.random.fold_in(streams_of[6], 71), 0),
        "kv_latent": noise(streams_of[1], (TOKENS, KVL + ROPE), 1.0, 6.0, ((0, 8), (1, 4))),
        "w_query": noise(streams_of[2], (QL, HEADS * (NOPE + ROPE)), QL ** -0.5, 0.15625, ((1, 4),)),
        "w_key": noise(streams_of[3], (KVL, HEADS * NOPE), KVL ** -0.5, 0.25, ((1, 4),)),
        "w_value": noise(streams_of[4], (KVL, HEADS * VDIM), KVL ** -0.5, 0.25, ((1, 4),)),
        "d_out": noise(streams_of[5], (TOKENS, HEADS * VDIM), 1.0, 6.0, ((0, 8), (1, 4))),
    }


def to_float(array):
    return array.astype(jnp.float32)


def shift_down(array):
    return jnp.concatenate([jnp.zeros_like(array[:1]), array[:-1]], 0)


def shift_up(array):
    return jnp.concatenate([array[1:], jnp.zeros_like(array[:1])], 0)


def reference(q_latent, kv_latent, w_query, w_key, w_value, d_out):
    group_count = N_HEAD
    per_group = HEAD_DEV
    block_count = N_CTX
    block_rows = TOK_DEV
    width = NOPE + ROPE
    softmax_scale = width ** -0.5
    query_w = w_query.reshape(QL, group_count, per_group * width).transpose(1, 0, 2)
    key_w = w_key.reshape(KVL, group_count, per_group * NOPE).transpose(1, 0, 2)
    value_w = w_value.reshape(KVL, group_count, per_group * VDIM).transpose(1, 0, 2)
    grad_groups = d_out.reshape(TOKENS, group_count, per_group * VDIM).transpose(1, 0, 2)
    rope_keys = kv_latent[:, KVL:].reshape(block_count, block_rows, ROPE)
    rope_all = jnp.concatenate([shift_down(rope_keys), rope_keys], 1)
    query_pos = jnp.arange(block_rows)[:, None]
    key_pos = jnp.arange(2 * block_rows)[None, :]
    block_idx = jnp.arange(block_count)[:, None, None]
    visible = jnp.where(key_pos < block_rows, block_idx > 0, key_pos - block_rows <= query_pos)
    latent_main = kv_latent[:, :KVL]

    def group_step(carry, inputs):
        wq_group, wk_group, wv_group, grad_group = inputs
        queries = jnp.dot(q_latent, wq_group, preferred_element_type=jnp.float32).astype(jnp.bfloat16)
        queries = queries.reshape(block_count, block_rows, per_group, width)
        keys_nope = jnp.dot(latent_main, wk_group, preferred_element_type=jnp.float32).astype(jnp.bfloat16)
        keys_nope = keys_nope.reshape(block_count, block_rows, per_group, NOPE)
        values = jnp.dot(latent_main, wv_group, preferred_element_type=jnp.float32).astype(jnp.bfloat16)
        values = values.reshape(block_count, block_rows, per_group, VDIM)
        keys_all = jnp.concatenate([shift_down(keys_nope), keys_nope], 1)
        values_all = jnp.concatenate([shift_down(values), values], 1)
        query_nope = queries[..., :NOPE]
        query_rope = queries[..., NOPE:]
        scores = jnp.einsum("nqhd,nkhd->nhqk", to_float(query_nope), to_float(keys_all))
        scores = (scores + jnp.einsum("nqhr,nkr->nhqk", to_float(query_rope), to_float(rope_all))) * softmax_scale
        mask = visible[:, None]
        scores = jnp.where(mask, scores, jnp.float32(-1e30))
        maxima = jnp.max(scores, -1, keepdims=True)
        expons = jnp.where(mask, jnp.exp(scores - maxima), jnp.float32(0.0))
        probs = expons / jnp.sum(expons, -1, keepdims=True)
        probs_b = probs.astype(jnp.bfloat16)
        output = jnp.einsum("nhqk,nkhd->nqhd", to_float(probs_b), to_float(values_all)).astype(jnp.bfloat16)
        grad_out = grad_group.reshape(block_count, block_rows, per_group, VDIM)
        dprob = jnp.einsum("nqhd,nkhd->nhqk", to_float(grad_out), to_float(values_all))
        row_dot = jnp.sum(to_float(grad_out) * to_float(output), -1).transpose(0, 2, 1)[..., None]
        dscore = (probs * (dprob - row_dot) * softmax_scale).astype(jnp.bfloat16)
        grad_qnope = jnp.einsum("nhqk,nkhd->nqhd", to_float(dscore), to_float(keys_all))
        grad_qrope = jnp.einsum("nhqk,nkr->nqhr", to_float(dscore), to_float(rope_all))
        grad_query = jnp.concatenate([grad_qnope, grad_qrope], -1).astype(jnp.bfloat16)
        grad_query = grad_query.reshape(TOKENS, per_group * width)
        grad_qgroup = jnp.dot(grad_query, wq_group.T, preferred_element_type=jnp.float32)
        grad_knope = jnp.einsum("nhqk,nqhd->nkhd", to_float(dscore), to_float(query_nope)).astype(jnp.bfloat16)
        grad_krope = jnp.einsum("nhqk,nqhr->nkhr", to_float(dscore), to_float(query_rope)).astype(jnp.bfloat16)
        grad_value = jnp.einsum("nhqk,nqhd->nkhd", to_float(probs_b), to_float(grad_out)).astype(jnp.bfloat16)

        def project(knope_part, krope_part, value_part):
            main_cols = jnp.dot(knope_part.reshape(TOKENS, per_group * NOPE), wk_group.T, preferred_element_type=jnp.float32)
            main_cols = main_cols + jnp.dot(value_part.reshape(TOKENS, per_group * VDIM), wv_group.T, preferred_element_type=jnp.float32)
            rope_cols = jnp.sum(to_float(krope_part), axis=2).reshape(TOKENS, ROPE)
            return jnp.concatenate([main_cols, rope_cols], -1)

        own_part = project(grad_knope[:, block_rows:], grad_krope[:, block_rows:], grad_value[:, block_rows:])
        next_part = project(shift_up(grad_knope[:, :block_rows]), shift_up(grad_krope[:, :block_rows]), shift_up(grad_value[:, :block_rows]))
        carry = (carry[0] + grad_qgroup, carry[1] + own_part + next_part)
        return carry, output.reshape(TOKENS, per_group * VDIM)

    start = (jnp.zeros((TOKENS, QL), jnp.float32), jnp.zeros((TOKENS, KVL + ROPE), jnp.float32))
    grads, outputs = lax.scan(group_step, start, (query_w, key_w, value_w, grad_groups))
    attn_out = outputs.transpose(1, 0, 2).reshape(TOKENS, HEADS * VDIM)
    return attn_out, grads[0], grads[1]
```

```python
import functools
import math

import jax
import jax.numpy as jnp
from jax import lax
from jax.experimental import pallas as pl
from jax.experimental.pallas import tpu as pltpu
from jax.sharding import PartitionSpec as P

KVL = 512
ROPE = 64
NOPE = 128
VDIM = 128
WIDTH = NOPE + ROPE
SCALE = WIDTH ** (-0.5)
F32 = jnp.float32
BF16 = jnp.bfloat16
MESH = pl.DeviceIdType.MESH


def nn(a, b):
    return jnp.dot(a, b, preferred_element_type=F32)


def nt(a, b):
    return lax.dot_general(a, b, (((1,), (1,)), ((), ())), preferred_element_type=F32)


def kernel(
    n_ctx, n_head,
    q_ref, kv_ref, do_ref, wq_hbm, wk_hbm, wv_hbm,
    out_ref, gq_ref, gkv_ref,
    wq, wk, wv, wkt, wvt, dot_t, q_in, kv_in, kv_prev, lat, lat_t, q_acc, q_t,
    keys, keys_t, values, values_t, gq_t, gk, gv, krope, back_out, back_in,
    rq_out, rq_in, rkv_out, rkv_in, gkv_own, gq_own,
    w_sem, kv_send, kv_recv, q_send, q_recv, p_send, p_recv,
    b_send, b_recv, rq_send, rq_recv, rkv_send, rkv_recv,
):
    ctx = lax.axis_index("ctx")
    me = lax.axis_index("head")
    rows, q_cols = q_ref.shape
    kv_cols = kv_ref.shape[1]
    heads = wk.shape[1] // NOPE
    after = lax.rem(ctx + 1, n_ctx)
    before = lax.rem(ctx + n_ctx - 1, n_ctx)
    order = sorted(range(1, n_head), key=lambda s: (min(s, n_head - s), s))

    loads = [
        pltpu.make_async_copy(src, dst, w_sem.at[i])
        for i, (src, dst) in enumerate(((wk_hbm, wk), (wv_hbm, wv), (wq_hbm, wq)))
    ]
    for load in loads:
        load.start()

    barrier = pltpu.get_barrier_semaphore()
    for s in range(1, n_head):
        pl.semaphore_signal(barrier, inc=1, device_id={"head": lax.rem(me + s, n_head)}, device_id_type=MESH)
    pl.semaphore_signal(barrier, inc=1, device_id={"ctx": after}, device_id_type=MESH)
    pl.semaphore_signal(barrier, inc=1, device_id={"ctx": before}, device_id_type=MESH)
    pl.semaphore_wait(barrier, n_head + 1)

    def send(src, dst, send_sem, recv_sem, device):
        copy = pltpu.make_async_remote_copy(
            src_ref=src, dst_ref=dst, send_sem=send_sem, recv_sem=recv_sem,
            device_id=device, device_id_type=MESH,
        )
        copy.start()
        return copy

    def peer(s):
        return {"head": lax.rem(me + s, n_head)}

    kv_copies = {s: send(kv_ref, kv_in.at[s], kv_send.at[s], kv_recv.at[s], peer(s)) for s in order}
    p_copies = {0: send(kv_ref, kv_prev.at[0], p_send.at[0], p_recv.at[0], {"ctx": after})}
    q_copies = {s: send(q_ref, q_in.at[s], q_send.at[s], q_recv.at[s], peer(s)) for s in order}

    @pl.loop(0, heads)
    def _(h):
        at = pl.multiple_of(h * VDIM, VDIM)
        dot_t[pl.ds(at, VDIM), :] = do_ref[:, pl.ds(at, VDIM)].T

    loads[0].wait()

    @pl.loop(0, heads)
    def _(h):
        at = pl.multiple_of(h * NOPE, NOPE)
        wkt[pl.ds(at, NOPE), :] = wk[:, pl.ds(at, NOPE)].T

    loads[1].wait()

    @pl.loop(0, heads)
    def _(h):
        at = pl.multiple_of(h * VDIM, VDIM)
        wvt[pl.ds(at, VDIM), :] = wv[:, pl.ds(at, VDIM)].T

    loads[2].wait()

    def add_queries(block, s, first):
        owner = lax.rem(me + n_head - s, n_head)
        at = pl.multiple_of(owner * q_cols, q_cols)
        tile = 2 * WIDTH

        @pl.loop(0, wq.shape[1] // tile)
        def _(j):
            cols = pl.ds(pl.multiple_of(j * tile, tile), tile)
            part = nn(block[...], wq[pl.ds(at, q_cols), cols])
            if first:
                q_acc[:, cols] = part
            else:
                q_acc[:, cols] += part

    add_queries(q_ref, 0, True)

    for s in order:
        kv_copies[s].wait_recv()
        p_copies[s] = send(kv_in.at[s], kv_prev.at[s], p_send.at[s], p_recv.at[s], {"ctx": after})

    def assemble(parts, row):
        width = n_head * kv_cols
        total = None
        total_t = None
        for s in range(n_head):
            owner = lax.rem(me + n_head - s, n_head)
            src = lax.broadcasted_iota(jnp.int32, (kv_cols, width), 0) + owner * kv_cols
            dst = lax.broadcasted_iota(jnp.int32, (kv_cols, width), 1)
            place = jnp.where(src == dst, F32(1.0), F32(0.0)).astype(BF16)
            src_t = lax.broadcasted_iota(jnp.int32, (ROPE, kv_cols), 1) + owner * kv_cols
            dst_t = lax.broadcasted_iota(jnp.int32, (ROPE, kv_cols), 0) + KVL
            place_t = jnp.where(src_t == dst_t, F32(1.0), F32(0.0)).astype(BF16)
            term = nn(parts[s], place)
            term_t = nt(place_t, parts[s])
            total = term if total is None else total + term
            total_t = term_t if total_t is None else total_t + term_t
        lat[row:row + rows, :] = total.astype(BF16)
        lat_t[:, row:row + rows] = total_t.astype(BF16)

    def expand(row):
        tile = 2 * NOPE

        @pl.loop(0, heads // 2)
        def _(j):
            cols = pl.ds(pl.multiple_of(j * tile, tile), tile)
            main = lat[row:row + rows, :KVL]
            keys[row:row + rows, cols] = nn(main, wk[:, cols]).astype(BF16)
            values[row:row + rows, cols] = nn(main, wv[:, cols]).astype(BF16)
            keys_t[cols, row:row + rows] = nt(wkt[cols, :], main).astype(BF16)
            values_t[cols, row:row + rows] = nt(wvt[cols, :], main).astype(BF16)

    assemble([kv_ref[...]] + [kv_in[s] for s in range(1, n_head)], rows)
    expand(rows)
    for s in range(n_head):
        p_copies[s].wait_recv()
    assemble([kv_prev[s] for s in range(n_head)], 0)
    expand(0)

    for s in order:
        q_copies[s].wait_recv()
        add_queries(q_in.at[s], s, False)

    @pl.loop(0, wq.shape[1] // NOPE)
    def _(j):
        at = pl.multiple_of(j * NOPE, NOPE)
        q_t[pl.ds(at, NOPE), :] = q_acc[:, pl.ds(at, NOPE)].astype(BF16).T

    krope[...] = jnp.zeros_like(krope)

    @pl.loop(0, heads)
    def _(h):
        at = pl.multiple_of(h * NOPE, NOPE)
        q_at = pl.ds(pl.multiple_of(h * WIDTH, WIDTH), WIDTH)
        cols = pl.ds(at, NOPE)
        query_t = q_t[q_at, :]
        key = jnp.concatenate([keys[:, cols], lat[:, KVL:]], 1)
        scores = nn(key, query_t)
        key_pos = lax.broadcasted_iota(jnp.int32, (2 * rows, rows), 0)
        query_pos = lax.broadcasted_iota(jnp.int32, (2 * rows, rows), 1)
        low = jnp.where(ctx == 0, rows, 0)
        visible = (key_pos >= low) & (key_pos - rows <= query_pos)
        scores = jnp.where(visible, scores, F32(-1e30))
        top = jnp.max(scores, 0, keepdims=True)
        expons = jnp.exp2((scores - top) * F32(SCALE * math.log2(math.e)))
        probs = expons * (F32(1.0) / jnp.sum(expons, 0, keepdims=True))
        probs_b = probs.astype(BF16)
        result = nn(values_t[cols, :], probs_b).astype(BF16)
        out_ref[cols, :] = result
        grad_out = dot_t[cols, :]
        row_dot = jnp.sum(grad_out.astype(F32) * result.astype(F32), 0, keepdims=True)
        dprob = nn(values[:, cols], grad_out)
        dscore = (probs * (dprob - row_dot) * F32(SCALE)).astype(BF16)
        key_t = jnp.concatenate([keys_t[cols, :], lat_t[...]], 0)
        gq_t[q_at, :] = nn(key_t, dscore).astype(BF16)
        gk[:, cols] = nt(dscore, query_t[:NOPE]).astype(BF16)
        krope[:, :rows] += nt(query_t[NOPE:], dscore[:rows]).astype(BF16).astype(F32)
        krope[:, rows:] += nt(query_t[NOPE:], dscore[rows:]).astype(BF16).astype(F32)
        gv[:, cols] = nt(probs_b, grad_out).astype(BF16)

    def project(row):
        return nt(wk[...], gk[row:row + rows, :]) + nt(wv[...], gv[row:row + rows, :])

    back_out[:KVL, :] = project(0).astype(BF16)
    back_out[KVL:, :] = krope[:, :rows].astype(BF16)
    back = send(back_out, back_in, b_send, b_recv, {"ctx": before})

    def query_part(s):
        at = pl.multiple_of(lax.rem(me + s, n_head) * q_cols, q_cols)
        return nn(wq[pl.ds(at, q_cols), :], gq_t[...])

    rq_copies = {}
    for s in order[::-1]:
        rq_out[s] = query_part(s).astype(BF16)
        rq_copies[s] = send(rq_out.at[s], rq_in.at[s], rq_send.at[s], rq_recv.at[s], peer(s))

    gkv_own[:KVL, :] = project(rows)
    gkv_own[KVL:, :] = krope[:, rows:]
    back.wait_recv()
    gkv_own[...] += back_in[...].astype(F32)

    def kv_part(s):
        at = pl.multiple_of(lax.rem(me + s, n_head) * kv_cols, kv_cols)
        return gkv_own[pl.ds(at, kv_cols), :]

    rkv_copies = {}
    for s in order[::-1]:
        rkv_out[s] = kv_part(s).astype(BF16)
        rkv_copies[s] = send(rkv_out.at[s], rkv_in.at[s], rkv_send.at[s], rkv_recv.at[s], peer(s))

    gq_own[...] = query_part(0)
    for s in order:
        rq_copies[s].wait_recv()
        gq_own[...] += rq_in[s].astype(F32)
    gq_ref[...] = gq_own[...]
    total = kv_part(0)
    for s in order:
        rkv_copies[s].wait_recv()
        total = total + rkv_in[s].astype(F32)
    gkv_ref[...] = total

    for s in order:
        kv_copies[s].wait_send()
        q_copies[s].wait_send()
        rq_copies[s].wait_send()
        rkv_copies[s].wait_send()
    for s in range(n_head):
        p_copies[s].wait_send()
    back.wait_send()


def on_device(n_ctx, n_head, q_latent, kv_latent, w_query, w_key, w_value, d_out):
    rows, q_cols = q_latent.shape
    kv_cols = kv_latent.shape[1]
    ql, qw = w_query.shape
    kw = w_key.shape[1]
    kvw = n_head * kv_cols
    vmem = pl.BlockSpec(memory_space=pltpu.VMEM)
    hbm = pl.BlockSpec(memory_space=pl.ANY)
    dma = pltpu.SemaphoreType.DMA
    out_t, gq_t, gkv_t = pl.pallas_call(
        functools.partial(kernel, n_ctx, n_head),
        out_shape=(
            jax.ShapeDtypeStruct((kw, rows), BF16),
            jax.ShapeDtypeStruct((q_cols, rows), F32),
            jax.ShapeDtypeStruct((kv_cols, rows), F32),
        ),
        in_specs=[vmem, vmem, vmem, hbm, hbm, hbm],
        out_specs=(vmem, vmem, vmem),
        scratch_shapes=[
            pltpu.VMEM((ql, qw), BF16),
            pltpu.VMEM((KVL, kw), BF16),
            pltpu.VMEM((KVL, kw), BF16),
            pltpu.VMEM((kw, KVL), BF16),
            pltpu.VMEM((kw, KVL), BF16),
            pltpu.VMEM((kw, rows), BF16),
            pltpu.VMEM((n_head, rows, q_cols), BF16),
            pltpu.VMEM((n_head, rows, kv_cols), BF16),
            pltpu.VMEM((n_head, rows, kv_cols), BF16),
            pltpu.VMEM((2 * rows, kvw), BF16),
            pltpu.VMEM((ROPE, 2 * rows), BF16),
            pltpu.VMEM((rows, qw), F32),
            pltpu.VMEM((qw, rows), BF16),
            pltpu.VMEM((2 * rows, kw), BF16),
            pltpu.VMEM((kw, 2 * rows), BF16),
            pltpu.VMEM((2 * rows, kw), BF16),
            pltpu.VMEM((kw, 2 * rows), BF16),
            pltpu.VMEM((qw, rows), BF16),
            pltpu.VMEM((2 * rows, kw), BF16),
            pltpu.VMEM((2 * rows, kw), BF16),
            pltpu.VMEM((ROPE, 2 * rows), F32),
            pltpu.VMEM((kvw, rows), BF16),
            pltpu.VMEM((kvw, rows), BF16),
            pltpu.VMEM((n_head, q_cols, rows), BF16),
            pltpu.VMEM((n_head, q_cols, rows), BF16),
            pltpu.VMEM((n_head, kv_cols, rows), BF16),
            pltpu.VMEM((n_head, kv_cols, rows), BF16),
            pltpu.VMEM((kvw, rows), F32),
            pltpu.VMEM((q_cols, rows), F32),
            dma((3,)),
            dma((n_head,)), dma((n_head,)),
            dma((n_head,)), dma((n_head,)),
            dma((n_head,)), dma((n_head,)),
            dma, dma,
            dma((n_head,)), dma((n_head,)),
            dma((n_head,)), dma((n_head,)),
        ],
        compiler_params=pltpu.CompilerParams(
            collective_id=0, has_side_effects=True, vmem_limit_bytes=60 * 1024 * 1024,
        ),
        name="latent_attention",
    )(q_latent, kv_latent, d_out, w_query, w_key, w_value)
    return out_t.T, gq_t.T, gkv_t.T


def solution(mesh):
    return jax.shard_map(
        functools.partial(on_device, mesh.shape["ctx"], mesh.shape["head"]),
        mesh=mesh,
        in_specs=(
            P("ctx", "head"),
            P("ctx", "head"),
            P(None, "head"),
            P(None, "head"),
            P(None, "head"),
            P("ctx", "head"),
        ),
        out_specs=(P("ctx", "head"), P("ctx", "head"), P("ctx", "head")),
        check_vma=False,
    )
```

```python
import functools
import math

import jax
import jax.numpy as jnp
from jax import lax
from jax.experimental import pallas as pl
from jax.experimental.pallas import tpu as pltpu
from jax.sharding import PartitionSpec as P

KVL = 512
ROPE = 64
NOPE = 128
VDIM = 128
WIDTH = NOPE + ROPE
SCALE = WIDTH ** (-0.5)
F32 = jnp.float32
BF16 = jnp.bfloat16
MESH = pl.DeviceIdType.MESH


def nn(a, b):
    return jnp.dot(a, b, preferred_element_type=F32)


def nt(a, b):
    return lax.dot_general(a, b, (((1,), (1,)), ((), ())), preferred_element_type=F32)


def kernel(
    n_ctx, n_head, chunks,
    q_ref, kv_ref, do_ref, wq_hbm, wk_hbm, wv_hbm,
    out_ref, gq_ref, gkv_ref,
    wq, wk, wv, wkt, wvt, dot_t, q_in, kv_in, kv_prev, lat, lat_t, q_acc, q_t,
    keys, keys_t, values, values_t, gq_t, gk, gv, gk_sum, gv_sum, kr_sum, krope, back_out, back_in,
    rq_out, rq_right, rq_left, rkv_out, rkv_right, rkv_left, gkv_own, stage_right, stage_left,
    bias, w_sem, kv_r, kv_l, kv_recv, q_r, q_l, q_recv, p_send, p_recv,
    b_send, b_recv, rq_send, rq_rr, rq_rl, rkv_send, rkv_rr, rkv_rl,
):
    ctx = lax.axis_index("ctx")
    me = lax.axis_index("head")
    last = n_head - 1
    rows, q_cols = q_ref.shape
    part_rows = rows // chunks
    kv_cols = kv_ref.shape[0]
    heads = wk.shape[1] // NOPE
    after = {"ctx": lax.rem(ctx + 1, n_ctx)}
    before = {"ctx": lax.rem(ctx + n_ctx - 1, n_ctx)}
    right = {"head": jnp.minimum(me + 1, last)}
    left = {"head": jnp.maximum(me - 1, 0)}
    has_right = me < last
    has_left = me > 0

    loads = [
        pltpu.make_async_copy(src, dst, w_sem.at[i])
        for i, (src, dst) in enumerate(((wk_hbm, wk), (wv_hbm, wv), (wq_hbm, wq)))
    ]
    for load in loads:
        load.start()

    barrier = pltpu.get_barrier_semaphore()

    @pl.when(has_right)
    def _():
        pl.semaphore_signal(barrier, inc=1, device_id=right, device_id_type=MESH)

    @pl.when(has_left)
    def _():
        pl.semaphore_signal(barrier, inc=1, device_id=left, device_id_type=MESH)

    pl.semaphore_signal(barrier, inc=1, device_id=after, device_id_type=MESH)
    pl.semaphore_signal(barrier, inc=1, device_id=before, device_id_type=MESH)
    pl.semaphore_wait(barrier, 2 + jnp.minimum(me, 1) + jnp.minimum(last - me, 1))

    def copy_of(src, dst, send_sem, recv_sem, device):
        return pltpu.make_async_remote_copy(
            src_ref=src, dst_ref=dst, send_sem=send_sem, recv_sem=recv_sem,
            device_id=device, device_id_type=MESH,
        )

    class Gather:
        def __init__(self, own, slots, send_r, send_l, recv):
            self.own, self.slots, self.recv = own, slots, recv
            self.send_r, self.send_l = send_r, send_l

        def moves(self, t, act):
            @pl.when(has_right & (me >= t))
            def _():
                owner = me - t
                src = self.own if t == 0 else self.slots(owner)
                act(copy_of(src, self.slots(owner), self.send_r(t), self.recv(owner), right))

            @pl.when(has_left & (me + t <= last))
            def _():
                owner = me + t
                src = self.own if t == 0 else self.slots(owner)
                act(copy_of(src, self.slots(owner), self.send_l(t), self.recv(owner), left))

        def start(self, t):
            if t < last:
                self.moves(t, lambda copy: copy.start())

        def each(self, t, act):
            @pl.when(me - 1 - t >= 0)
            def _():
                act(me - 1 - t)

            @pl.when(me + 1 + t <= last)
            def _():
                act(me + 1 + t)

        def arrive(self, t, act=None):
            def wait(owner):
                slot = self.slots(owner)
                copy_of(slot, slot, self.send_r(0), self.recv(owner), right).wait_recv()
                if act is not None:
                    act(owner)

            self.each(t, wait)
            self.start(t + 1)

        def finish(self):
            for t in range(last):
                self.moves(t, lambda copy: copy.wait_send())

    def pass_on(owner, src):
        copy_of(src, kv_prev.at[owner], p_send.at[owner], p_recv.at[owner], after).start()

    kv_gather = Gather(kv_ref, lambda i: kv_in.at[i], lambda t: kv_r.at[t], lambda t: kv_l.at[t], lambda i: kv_recv.at[i])
    q_gathers = [
        Gather(
            q_ref.at[pl.ds(c * part_rows, part_rows), :],
            lambda i, c=c: q_in.at[c, i],
            lambda t, c=c: q_r.at[c, t],
            lambda t, c=c: q_l.at[c, t],
            lambda i, c=c: q_recv.at[c, i],
        )
        for c in range(chunks)
    ]
    kv_gather.start(0)
    pass_on(me, kv_ref)
    for gather in q_gathers:
        gather.start(0)
    kv_in[me] = kv_ref[...]

    key_pos = lax.broadcasted_iota(jnp.int32, (2 * rows, rows), 0)
    query_pos = lax.broadcasted_iota(jnp.int32, (2 * rows, rows), 1)
    low = jnp.where(ctx == 0, rows, 0)
    visible = (key_pos >= low) & (key_pos - rows <= query_pos)
    bias[...] = jnp.where(visible, F32(0.0), F32(-1e30))
    loads[0].wait()

    @pl.loop(0, heads)
    def _(h):
        at = pl.multiple_of(h * NOPE, NOPE)
        wkt[pl.ds(at, NOPE), :] = wk[:, pl.ds(at, NOPE)].T

    def kv_step(t):
        kv_gather.arrive(t, lambda owner: pass_on(owner, kv_in.at[owner]))

    def q_step(c, t):
        q_gathers[c].arrive(t)

    kv_step(0)
    loads[1].wait()

    @pl.loop(0, heads)
    def _(h):
        at = pl.multiple_of(h * VDIM, VDIM)
        wvt[pl.ds(at, VDIM), :] = wv[:, pl.ds(at, VDIM)].T

    def add_queries(c, block, owner, first=False):
        at = pl.multiple_of(owner * q_cols, q_cols)
        span = pl.ds(c * part_rows, part_rows)
        tile = 2 * WIDTH

        @pl.loop(0, wq.shape[1] // tile)
        def _(j):
            cols = pl.ds(pl.multiple_of(j * tile, tile), tile)
            part = nn(block[...], wq[pl.ds(at, q_cols), cols])
            if first:
                q_acc[span, cols] = part
            else:
                q_acc[span, cols] += part

    def add_arrived(c, t):
        q_gathers[c].each(t, lambda owner: add_queries(c, q_in.at[c, owner], owner))

    def assemble(parts, row):
        width = n_head * kv_cols
        total = None
        for i in range(n_head):
            dst = lax.broadcasted_iota(jnp.int32, (width, kv_cols), 0)
            src = lax.broadcasted_iota(jnp.int32, (width, kv_cols), 1) + i * kv_cols
            place = jnp.where(src == dst, F32(1.0), F32(0.0)).astype(BF16)
            term = nn(place, parts[i])
            total = term if total is None else total + term
        total = total.astype(BF16)
        span = slice(row, row + rows)
        lat_t[:, span] = total
        lat[span, :KVL] = total[:KVL].T
        lat[span, KVL:] = total[KVL:].T

    def expand(row):
        tile = 2 * NOPE
        span = slice(row, row + rows)

        @pl.loop(0, heads // 2)
        def _(j):
            cols = pl.ds(pl.multiple_of(j * tile, tile), tile)
            main = lat[span, :KVL]
            main_t = lat_t[:KVL, span]
            keys[span, cols] = nn(main, wk[:, cols]).astype(BF16)
            values[span, cols] = nn(main, wv[:, cols]).astype(BF16)
            keys_t[cols, span] = nn(wkt[cols, :], main_t).astype(BF16)
            values_t[cols, span] = nn(wvt[cols, :], main_t).astype(BF16)

    def finish_queries(c):
        @pl.loop(0, wq.shape[1] // NOPE)
        def _(j):
            at = pl.multiple_of(j * NOPE, NOPE)
            span = slice(c * part_rows, (c + 1) * part_rows)
            q_t[pl.ds(at, NOPE), span] = q_acc[span, pl.ds(at, NOPE)].astype(BF16).T

    if last > 0:
        q_step(0, 0)

    @pl.loop(0, heads)
    def _(h):
        at = pl.multiple_of(h * VDIM, VDIM)
        dot_t[pl.ds(at, VDIM), :] = do_ref[:, pl.ds(at, VDIM)].T

    loads[2].wait()
    for c in range(chunks):
        add_queries(c, q_ref.at[pl.ds(c * part_rows, part_rows), :], me, True)
    for t in range(1, last):
        kv_step(t)
        add_arrived(0, t - 1)
        if t < last - 1:
            q_step(0, t)
    assemble([kv_in[i] for i in range(n_head)], rows)
    expand(rows)
    for i in range(n_head):
        copy_of(kv_ref, kv_prev.at[i], p_send.at[i], p_recv.at[i], after).wait_recv()
    assemble([kv_prev[i] for i in range(n_head)], 0)
    expand(0)
    if last > 1:
        q_step(0, last - 1)
    if last > 0:
        add_arrived(0, last - 1)
    finish_queries(0)
    krope[...] = jnp.zeros_like(krope)

    def attend(c, h):
        seen = rows + (c + 1) * part_rows
        span = slice(c * part_rows, (c + 1) * part_rows)
        at = pl.multiple_of(h * NOPE, NOPE)
        q_at = pl.ds(pl.multiple_of(h * WIDTH, WIDTH), WIDTH)
        cols = pl.ds(at, NOPE)
        query_t = q_t[q_at, span]
        key = jnp.concatenate([keys[:seen, cols], lat[:seen, KVL:]], 1)
        scores = nn(key, query_t)
        scores = scores + bias[:seen, span]
        top = jnp.max(scores, 0, keepdims=True)
        expons = jnp.exp2((scores - top) * F32(SCALE * math.log2(math.e)))
        probs = expons * (F32(1.0) / jnp.sum(expons, 0, keepdims=True))
        probs_b = probs.astype(BF16)
        result = nn(values_t[cols, :seen], probs_b).astype(BF16)
        out_ref[cols, span] = result
        grad_out = dot_t[cols, span]
        row_dot = jnp.sum(grad_out.astype(F32) * result.astype(F32), 0, keepdims=True)
        dprob = nn(values[:seen, cols], grad_out)
        dscore = (probs * (dprob - row_dot) * F32(SCALE)).astype(BF16)
        key_t = jnp.concatenate([keys_t[cols, :seen], lat_t[KVL:, :seen]], 0)
        gq_t[q_at, span] = nn(key_t, dscore).astype(BF16)
        g_key = nt(dscore, query_t[:NOPE])
        g_rope = nt(query_t[NOPE:], dscore)
        g_value = nt(probs_b, grad_out)
        if c > 0:
            before_rows = rows + c * part_rows
            g_key = jnp.concatenate([g_key[:before_rows] + gk_sum[:, cols], g_key[before_rows:]], 0)
            g_value = jnp.concatenate([g_value[:before_rows] + gv_sum[:, cols], g_value[before_rows:]], 0)
            g_rope = jnp.concatenate([g_rope[:, :before_rows] + kr_sum[h], g_rope[:, before_rows:]], 1)
        if c + 1 < chunks:
            gk_sum[:, cols] = g_key
            gv_sum[:, cols] = g_value
            kr_sum[h] = g_rope
        else:
            gk[:, cols] = g_key.astype(BF16)
            gv[:, cols] = g_value.astype(BF16)
            krope[...] += g_rope.astype(BF16).astype(F32)

    def attention(c, hooks):
        groups = max(1, len(hooks) + 1)
        edges = [heads * g // groups for g in range(groups + 1)]
        for g in range(groups):
            @pl.loop(edges[g] // UNROLL, edges[g + 1] // UNROLL)
            def _(h):
                for u in range(UNROLL):
                    attend(c, h * UNROLL + u)

            if g < len(hooks):
                hooks[g]()

    class Reduce:
        def __init__(self, part, out, in_right, in_left, send, recv_right, recv_left, stages):
            self.part, self.out, self.send = part, out, send
            self.ways = (
                (in_right, recv_right, right, stages[0], has_left),
                (in_left, recv_left, left, stages[1], has_right),
            )

        def step(self, tick):
            for way, (slots, recv, device, stage, joined) in enumerate(self.ways):
                lag = me if way == 0 else last - me
                owner = last - (tick - lag) if way == 0 else tick - lag

                @pl.when(tick >= lag)
                def _():
                    stage[...] = self.part(owner)

                    @pl.when(joined)
                    def _():
                        copy_of(slots(owner), slots(owner), self.send(owner), recv(owner), device).wait_recv()
                        stage[...] += slots(owner)[...].astype(F32)

                    self.out(owner)[...] = stage[...].astype(BF16)
                    copy_of(self.out(owner), slots(owner), self.send(owner), recv(owner), device).start()

        def total(self, stage):
            stage[...] = self.part(me)
            for slots, recv, device, _, joined in self.ways:
                @pl.when(joined)
                def _():
                    copy_of(slots(me), slots(me), self.send(me), recv(me), device).wait_recv()
                    stage[...] += slots(me)[...].astype(F32)

        def finish(self):
            for i in range(n_head):
                @pl.when(me != i)
                def _():
                    slot = self.out(i)
                    copy_of(slot, slot, self.send(i), self.send(i), right).wait_send()

    def query_part(c):
        def part(owner):
            at = pl.multiple_of(owner * q_cols, q_cols)
            return nn(wq[pl.ds(at, q_cols), :], gq_t[:, c * part_rows:(c + 1) * part_rows])

        return part

    def kv_part(owner):
        return gkv_own[pl.ds(pl.multiple_of(owner * kv_cols, 8), kv_cols), :]

    q_reduces = [
        Reduce(
            query_part(c),
            lambda i, c=c: rq_out.at[c, i],
            lambda i, c=c: rq_right.at[c, i],
            lambda i, c=c: rq_left.at[c, i],
            lambda i, c=c: rq_send.at[c, i],
            lambda i, c=c: rq_rr.at[c, i],
            lambda i, c=c: rq_rl.at[c, i],
            (stage_right, stage_left),
        )
        for c in range(chunks)
    ]
    kv_stage = (gkv_ref, gkv_ref)
    kv_reduce = Reduce(
        kv_part,
        lambda i: rkv_out.at[i],
        lambda i: rkv_right.at[i],
        lambda i: rkv_left.at[i],
        lambda i: rkv_send.at[i],
        lambda i: rkv_rr.at[i],
        lambda i: rkv_rl.at[i],
        kv_stage,
    )

    for c in range(chunks):
        hooks = []
        if c + 1 < chunks:
            hooks += [functools.partial(q_step, c + 1, t) for t in range(last)]
        if c > 0:
            hooks += [functools.partial(q_reduces[c - 1].step, t) for t in range(last)]
        attention(c, hooks)
        if c + 1 < chunks:
            for t in range(last):
                add_arrived(c + 1, t)
            finish_queries(c + 1)

    def project(row):
        return nt(wk[...], gk[row:row + rows, :]) + nt(wv[...], gv[row:row + rows, :])

    final = q_reduces[chunks - 1]
    if last > 0:
        final.step(0)
    back_out[:KVL, :] = project(0).astype(BF16)
    back_out[KVL:, :] = krope[:, :rows].astype(BF16)
    back = copy_of(back_out, back_in, b_send, b_recv, before)
    back.start()
    gkv_own[:KVL, :] = project(rows)
    gkv_own[KVL:, :] = krope[:, rows:]
    if last > 1:
        final.step(1)
    back.wait_recv()
    gkv_own[...] += back_in[...].astype(F32)
    for t in range(last):
        kv_reduce.step(t)
        if t + 2 < last:
            final.step(t + 2)

    for c in range(chunks):
        q_reduces[c].total(stage_right)
        gq_ref[:, c * part_rows:(c + 1) * part_rows] = stage_right[...]
    kv_reduce.total(gkv_ref)

    kv_gather.finish()
    kv_reduce.finish()
    for c in range(chunks):
        q_gathers[c].finish()
        q_reduces[c].finish()
    for i in range(n_head):
        copy_of(kv_ref, kv_prev.at[i], p_send.at[i], p_recv.at[i], after).wait_send()
    back.wait_send()


CHUNKS = 1
UNROLL = 2


def on_device(n_ctx, n_head, q_latent, kv_latent, w_query, w_key, w_value, d_out):
    rows, q_cols = q_latent.shape
    kv_cols = kv_latent.shape[1]
    ql, qw = w_query.shape
    kw = w_key.shape[1]
    kvw = n_head * kv_cols
    heads = kw // NOPE
    part_rows = rows // CHUNKS
    held = 2 * rows - part_rows if CHUNKS > 1 else 8
    vmem = pl.BlockSpec(memory_space=pltpu.VMEM)
    hbm = pl.BlockSpec(memory_space=pl.ANY)
    dma = pltpu.SemaphoreType.DMA
    some = (n_head,)
    each = (CHUNKS, n_head)
    out_t, gq_t, gkv_t = pl.pallas_call(
        functools.partial(kernel, n_ctx, n_head, CHUNKS),
        out_shape=(
            jax.ShapeDtypeStruct((kw, rows), BF16),
            jax.ShapeDtypeStruct((q_cols, rows), F32),
            jax.ShapeDtypeStruct((kv_cols, rows), F32),
        ),
        in_specs=[vmem, vmem, vmem, hbm, hbm, hbm],
        out_specs=(vmem, vmem, vmem),
        scratch_shapes=[
            pltpu.VMEM((ql, qw), BF16),
            pltpu.VMEM((KVL, kw), BF16),
            pltpu.VMEM((KVL, kw), BF16),
            pltpu.VMEM((kw, KVL), BF16),
            pltpu.VMEM((kw, KVL), BF16),
            pltpu.VMEM((kw, rows), BF16),
            pltpu.VMEM((CHUNKS, n_head, part_rows, q_cols), BF16),
            pltpu.VMEM((n_head, kv_cols, rows), BF16),
            pltpu.VMEM((n_head, kv_cols, rows), BF16),
            pltpu.VMEM((2 * rows, kvw), BF16),
            pltpu.VMEM((kvw, 2 * rows), BF16),
            pltpu.VMEM((rows, qw), F32),
            pltpu.VMEM((qw, rows), BF16),
            pltpu.VMEM((2 * rows, kw), BF16),
            pltpu.VMEM((kw, 2 * rows), BF16),
            pltpu.VMEM((2 * rows, kw), BF16),
            pltpu.VMEM((kw, 2 * rows), BF16),
            pltpu.VMEM((qw, rows), BF16),
            pltpu.VMEM((2 * rows, kw), BF16),
            pltpu.VMEM((2 * rows, kw), BF16),
            pltpu.VMEM((held, kw), F32),
            pltpu.VMEM((held, kw), F32),
            pltpu.VMEM((heads, ROPE, held), F32),
            pltpu.VMEM((ROPE, 2 * rows), F32),
            pltpu.VMEM((kvw, rows), BF16),
            pltpu.VMEM((kvw, rows), BF16),
            pltpu.VMEM((CHUNKS, n_head, q_cols, part_rows), BF16),
            pltpu.VMEM((CHUNKS, n_head, q_cols, part_rows), BF16),
            pltpu.VMEM((CHUNKS, n_head, q_cols, part_rows), BF16),
            pltpu.VMEM((n_head, kv_cols, rows), BF16),
            pltpu.VMEM((n_head, kv_cols, rows), BF16),
            pltpu.VMEM((n_head, kv_cols, rows), BF16),
            pltpu.VMEM((kvw, rows), F32),
            pltpu.VMEM((q_cols, part_rows), F32),
            pltpu.VMEM((q_cols, part_rows), F32),
            pltpu.VMEM((2 * rows, rows), F32),
            dma((3,)),
            dma(some), dma(some), dma(some),
            dma(each), dma(each), dma(each),
            dma(some), dma(some),
            dma, dma,
            dma(each), dma(each), dma(each),
            dma(some), dma(some), dma(some),
        ],
        compiler_params=pltpu.CompilerParams(
            collective_id=0, has_side_effects=True, vmem_limit_bytes=62 * 1024 * 1024,
        ),
        name="latent_attention",
    )(q_latent, kv_latent.T, d_out, w_query, w_key, w_value)
    return out_t.T, gq_t.T, gkv_t.T


def solution(mesh):
    return jax.shard_map(
        functools.partial(on_device, mesh.shape["ctx"], mesh.shape["head"]),
        mesh=mesh,
        in_specs=(
            P("ctx", "head"),
            P("ctx", "head"),
            P(None, "head"),
            P(None, "head"),
            P(None, "head"),
            P("ctx", "head"),
        ),
        out_specs=(P("ctx", "head"), P("ctx", "head"), P("ctx", "head")),
        check_vma=False,
    )
```
